256 devices in a mesh: clu: 32 (over z, x_hi, core), doc: 8 (over y, x_lo).
Axes of the slice: x: 4 (x_hi: 2, x_lo: 2; x = x_hi * 2 + x_lo), y: 4, z: 8, core: 2. Of those that a mesh axis runs over, the one named last changes fastest.
Arguments:
- docs: bfloat16 [65536, 768], P(('clu', 'doc')), may hold values from -6 to 6
- centroids: bfloat16 [11008, 768], P('doc', 'clu'), may hold values from -6 to 6
- assigned: int32 [65536], P(('clu', 'doc')), may hold values from 0 to 11007
Outputs:
- nearest: float32 [65536], P(('clu', 'doc'))
- assigned_dist: float32 [65536], P(('clu', 'doc'))
The draws below stay inside these ranges and needn't reach their ends.
Inputs may be any that keep to these rules, and one draw needn't show every extreme that they name: `assigned`: cluster ids.
All inputs are finite; a program needn't handle non-finite values.
Results may differ from the reference program's by a relative error of at most 0.0003.
Values may be sent and summed in bfloat16 or wider, within the bound.
No kernel may reach another device: no remote copies, remote signals or barrier semaphores. Data moves between devices by JAX's collectives and lax.ppermute only.
A program may use at most 64 MiB of HBM per device.

```python
import jax
import jax.numpy as jnp
from jax import lax

D = 768
K = 11008
N = 65536
N_CLU = 32


def touch_ends(entries, stream_key, least, top_value):
    longest = entries.shape.index(max(entries.shape))
    spots = []
    for shift in (0, 1):
        where = [jax.random.randint(jax.random.fold_in(stream_key, axis), (), 0, length) for axis, length in enumerate(entries.shape)]
        where[longest] = (where[longest] + shift) % entries.shape[longest]
        spots.append(tuple(where))
    return entries.at[spots[0]].set(least).at[spots[1]].set(top_value)


def block_scale(key, dims, pieces, least, largest):
    def one(dim, blocks):
        steps = jax.random.uniform(jax.random.fold_in(jax.random.fold_in(key, 6), dim), (blocks,), jnp.float32, least / len(pieces), largest / len(pieces))
        return jnp.repeat(jnp.exp(steps), dims[dim] // blocks).reshape((-1,) + (1,) * (len(dims) - dim - 1))

    gain = one(*pieces[0])
    for cut in pieces[1:]:
        gain = gain * one(*cut)
    return gain


def centred(own_key, dims, spread, bound, shards=(), dtype=jnp.bfloat16):
    level = block_scale(own_key, dims, shards, -0.22, 0.18) if shards else 1.0
    values = jax.random.normal(own_key, dims, jnp.float32) * spread * level
    return jnp.minimum(jnp.maximum(values, -bound), bound).astype(dtype)


def setup_inputs(seed: int = 0) -> dict:
    splits = jax.random.split(jax.random.key(seed), 4)
    return {
        "docs": centred(splits[0], (N, D), 1.0, 6.0, ((0, 256),)),
        "centroids": centred(splits[1], (K, D), 1.0, 6.0, ((0, 8), (1, 32))),
        "assigned": touch_ends(jax.random.randint(splits[2], (N,), 0, K), jax.random.fold_in(splits[2], 1), 0, K - 1).astype(jnp.int32),
    }


epsilon = 1e-06

def reference(docs, centroids, assigned):
    cent_wide = centroids.astype(jnp.float32)
    scale_c = lax.rsqrt(lax.optimization_barrier(jnp.sum(cent_wide * cent_wide, 1)) + epsilon)
    features = docs.shape[1]

    def score_block(inputs):
        doc_rows, doc_ids = inputs
        row_wide = doc_rows.astype(jnp.float32)
        scale_x = lax.rsqrt(lax.optimization_barrier(jnp.sum(row_wide * row_wide, 1)) + epsilon)
        products = jnp.dot(doc_rows, centroids.T, preferred_element_type=jnp.float32)
        distance = 1.0 - products * scale_x[:, None] * scale_c[None, :]
        nearest = lax.optimization_barrier(jnp.min(distance, 1))
        chosen = jnp.take_along_axis(distance, doc_ids[:, None].astype(jnp.int32), axis=1)[:, 0]
        return (nearest, chosen)
    nearest, chosen = lax.map(score_block, (docs.reshape(N_CLU, -1, features), assigned.reshape(N_CLU, -1)))
    return (nearest.reshape(-1), chosen.reshape(-1))
```

```python
import itertools

import jax
import jax.numpy as jnp
from jax import lax
from jax.experimental import pallas as pl
from jax.experimental.pallas import tpu as pltpu
from jax.sharding import Mesh
from jax.sharding import PartitionSpec as P

AXES = ("z", "xh", "c", "y", "xl")
DOC = ("y", "xl")
CLU = ("z", "xh", "c")
ALL = ("z", "xh", "c", "y", "xl")


epsilon = 1e-06
LOWEST = -3.0e38
LANES = 128
CHUNK = 256


def hops(sizes, move):
    pairs = []
    for here in itertools.product(*(range(n) for n in sizes)):
        there = move(*here)
        index = [0, 0]
        for n, a, b in zip(sizes, here, there):
            index = [index[0] * n + a, index[1] * n + b % n]
        pairs.append(tuple(index))
    return pairs


def way(c):
    return 1 - 2 * c


def along_y(step):
    return lambda z, xh, c, y, xl: (z, xh, c, y + step * way(c), xl)


def along_z(step):
    return lambda z, xh, c, y, xl: (z + step * way(c), xh, c, y, xl)


def across_x(z, xh, c, y, xl):
    x = 2 * xh + xl
    other = x + 1 if (x + c) % 2 == 0 else x - 1
    other %= 4
    return (z, other // 2, c, y, other % 2)


def far_x(z, xh, c, y, xl):
    return (z, xh + 1, c, y, xl)


def other_core(z, xh, c, y, xl):
    return (z, xh, c + 1, y, xl)


def assemble(own, traded, w_ref, scale_ref):
    z, xh, c = (lax.axis_index(name) for name in CLU)
    deep, wide = w_ref.shape
    rows = own[0][0].shape[0] // 2
    count = own[0][0].shape[1]
    w_ref[:, count - count % LANES :] = jnp.zeros((deep, wide - count + count % LANES), w_ref.dtype)
    for core, pieces in ((c, own), (1 - c, traded)):
        for ref, at, step in pieces:
            level = lax.rem(z - way(core) * step + 8, 8)
            for side in (0, 1):
                half = side + xh - 2 * side * xh
                start = ((level * 2 + half) * 2 + core) * rows
                w_ref[pl.ds(pl.multiple_of(start, 8), rows), :count] = ref[at + side * rows : at + (side + 1) * rows, :]
    whole = w_ref[...].astype(jnp.float32)
    scale_ref[...] = lax.rsqrt(jnp.sum(whole * whole, 0, keepdims=True) + epsilon)


def assemble_kernel(*refs):
    *pieces, w_ref, scale_ref = refs
    own = [(ref, 0, step) for ref, step in zip(pieces, STEPS)]
    height = pieces[0].shape[0]
    traded, at = [], 0
    for ref in pieces[8:]:
        for k in range(ref.shape[0] // height):
            traded.append((ref, k * height, STEPS[at]))
            at += 1
    assemble(own, traded, w_ref, scale_ref)


STEPS = (0, 1, -1, 2, -2, 3, -3, 4)


def score_kernel(count, *refs):
    *blocks, w_ref, scale_ref, out_ref, rows_ref, ids_ref, best_ref, chosen_ref = refs
    first = (lax.axis_index("y") * 2 + lax.axis_index("xl")) * count
    size = out_ref.shape[1]
    for k, block in enumerate(blocks):
        here = slice(k * size, (k + 1) * size)
        rows_ref[here, :] = block[:size, :]
        digits = block[size : size + 8, :size].astype(jnp.float32)
        ids = digits[0:1] * 128.0 + digits[1:2] - first.astype(jnp.float32)
        ids_ref[here, :] = jnp.broadcast_to(ids, (LANES, size)).T
    wide = w_ref.shape[1]
    lane = lax.broadcasted_iota(jnp.int32, (1, LANES), 1).astype(jnp.float32)
    for start in range(0, wide, CHUNK):
        stop = min(start + CHUNK, wide)
        products = jnp.dot(rows_ref[...], w_ref[:, start:stop], preferred_element_type=jnp.float32)
        scaled = products * scale_ref[:, start:stop]
        for at in range(start, stop, LANES):
            part = scaled[:, at - start : at - start + LANES]
            seen = part
            if at + LANES > count:
                seen = jnp.where(lane < float(count - at), part, LOWEST)
            hit = ids_ref[...] == lane + float(at)
            if at == 0:
                best_ref[...] = seen
                chosen_ref[...] = jnp.where(hit, seen, LOWEST)
            else:
                best_ref[...] = jnp.maximum(best_ref[...], seen)
                chosen_ref[...] = jnp.where(hit, seen, chosen_ref[...])
    for k in range(len(blocks)):
        here = slice(k * size, (k + 1) * size)
        out_ref[2 * k : 2 * k + 1, :] = jnp.max(best_ref[here, :].T, 0, keepdims=True)
        out_ref[2 * k + 1 : 2 * k + 2, :] = jnp.max(chosen_ref[here, :].T, 0, keepdims=True)


def score(blocks, w, scale, count, size):
    n = len(blocks)
    vmem = pl.BlockSpec(memory_space=pltpu.VMEM)
    return pl.pallas_call(
        lambda *refs: score_kernel(count, *refs),
        name="score",
        out_shape=jax.ShapeDtypeStruct((2 * n, size), jnp.float32),
        in_specs=[vmem] * (n + 2),
        out_specs=vmem,
        scratch_shapes=[
            pltpu.VMEM((n * size, w.shape[0]), jnp.bfloat16),
            pltpu.VMEM((n * size, LANES), jnp.float32),
            pltpu.VMEM((n * size, LANES), jnp.float32),
            pltpu.VMEM((n * size, LANES), jnp.float32),
        ],
        cost_estimate=pl.CostEstimate(
            flops=2 * n * size * w.shape[0] * w.shape[1], bytes_accessed=n * size * w.shape[0] * 2, transcendentals=0
        ),
    )(*blocks, w, scale)


def whole_block(own, traded):
    vmem = pl.BlockSpec(memory_space=pltpu.VMEM)
    height, count = own[0].shape
    wide = -(-count // LANES) * LANES
    return pl.pallas_call(
        assemble_kernel,
        name="assemble",
        out_shape=(
            jax.ShapeDtypeStruct((16 * height, wide), jnp.bfloat16),
            jax.ShapeDtypeStruct((1, wide), jnp.float32),
        ),
        in_specs=[vmem] * (len(own) + len(traded)),
        out_specs=(vmem, vmem),
        cost_estimate=pl.CostEstimate(flops=32 * height * wide, bytes_accessed=64 * height * wide, transcendentals=0),
    )(*own, *traded)


def on_device(sizes, docs, centroids, assigned):
    def send(value, move, name):
        with jax.named_scope(name):
            return lax.ppermute(value, ALL, hops(sizes, move))

    size, _ = docs.shape
    count = centroids.shape[0]
    mine = centroids.T
    theirs = send(mine, far_x, "h0")
    digits = jnp.stack([assigned >> 7, assigned & 127]).astype(jnp.bfloat16)
    tail = jnp.pad(digits, ((0, 6), (0, docs.shape[1] - size)))
    own = jnp.concatenate([docs, tail])
    slices = [jnp.concatenate([mine, theirs])]
    ahead = back = slices[0]
    rows = [own]
    rows.append(send(own, along_y(1), "y0"))
    rows.append(send(own, along_y(-1), "y1"))
    rows.append(send(rows[1], along_y(1), "y2"))
    pairs = [send(r, across_x, f"x{k}") for k, r in enumerate(rows)]
    for k in range(3):
        ahead = send(ahead, along_z(1), f"a{k}")
        back = send(back, along_z(-1), f"b{k}")
        slices += [ahead, back]
    slices.append(send(ahead, along_z(1), "a3"))
    traded = [
        send(jnp.concatenate(slices[:5]), other_core, "c0"),
        send(jnp.concatenate(slices[5:7]), other_core, "c1"),
        send(slices[7], other_core, "c2"),
    ]
    w, scale = whole_block(slices, traded)
    wide = docs.astype(jnp.float32)
    scale_x = lax.rsqrt(jnp.sum(wide * wide, 1) + epsilon)
    away = send(score(pairs, w, scale, count, size), across_x, "r0")
    here = jnp.maximum(score(rows, w, scale, count, size), away)
    total = here[0:2]
    for k, move in ((1, along_y(-1)), (2, along_y(1)), (3, along_y(2))):
        total = jnp.maximum(total, send(here[2 * k : 2 * k + 2], move, f"s{k}"))
    nearest, chosen = (1.0 - total[k] * scale_x for k in (0, 1))
    return (nearest, chosen)


def solution(mesh):
    clu, doc = mesh.shape["clu"], mesh.shape["doc"]
    sizes = (clu // 4, 2, 2, doc // 2, 2)
    torus = Mesh(mesh.devices.reshape(sizes), AXES)
    placed = (P(ALL, None), P(DOC, CLU), P(ALL))
    return jax.shard_map(
        lambda *args: on_device(sizes, *args), mesh=torus, in_specs=placed, out_specs=(P(ALL), P(ALL)), check_vma=False
    )
```

```python
import itertools

import jax
import jax.numpy as jnp
from jax import lax
from jax.experimental import pallas as pl
from jax.experimental.pallas import tpu as pltpu
from jax.sharding import Mesh
from jax.sharding import PartitionSpec as P

AXES = ("z", "xh", "c", "y", "xl")
DOC = ("y", "xl")
CLU = ("z", "xh", "c")
ALL = ("z", "xh", "c", "y", "xl")


epsilon = 1e-06
LOWEST = -3.0e38
LANES = 128
CHUNK = 256
SCORE_VMEM = 16 << 20
ASSEMBLE_VMEM = 16 << 20
JOIN_VMEM = 4 << 20
STEPS = (0, 1, -1, 2, -2, 3, -3, 4)


def hops(sizes, move):
    pairs = []
    for here in itertools.product(*(range(n) for n in sizes)):
        there = move(*here)
        index = [0, 0]
        for n, a, b in zip(sizes, here, there):
            index = [index[0] * n + a, index[1] * n + b % n]
        pairs.append(tuple(index))
    return pairs


def way(c):
    return 1 - 2 * c


def along_z(step):
    return lambda z, xh, c, y, xl: (z + step * way(c), xh, c, y, xl)


def across_x(z, xh, c, y, xl):
    x = 2 * xh + xl
    other = x + 1 if (x + c) % 2 == 0 else x - 1
    other %= 4
    return (z, other // 2, c, y, other % 2)


def far_x(z, xh, c, y, xl):
    return (z, xh + 1, c, y, xl)


def first_y(z, xh, c, y, xl):
    return (z, xh, c, (3 - y) if c else y + 1 - 2 * (y % 2), xl)


def second_y(z, xh, c, y, xl):
    return (z, xh, c, y + 1 - 2 * (y % 2) if c else (3 - y), xl)


def both_ways(*place):
    return second_y(*across_x(*place))


def other_core(z, xh, c, y, xl):
    return (z, xh, c + 1, y, xl)


def assemble_kernel(*refs):
    *pieces, early_ref, late_ref, w_ref, scale_ref = refs
    z, xh, c = (lax.axis_index(name) for name in CLU)
    deep, wide = w_ref.shape
    height, count = pieces[0].shape
    rows = height // 2
    w_ref[:, count - count % LANES :] = jnp.zeros((deep, wide - count + count % LANES), w_ref.dtype)
    traded = [(ref, k * height) for ref in (early_ref, late_ref) for k in range(ref.shape[0] // height)]
    for core, arrived in ((c, [(ref, 0) for ref in pieces]), (1 - c, traded)):
        for step, (ref, at) in zip(STEPS, arrived):
            level = lax.rem(z - way(core) * step + 8, 8)
            for side in (0, 1):
                half = side + xh - 2 * side * xh
                start = ((level * 2 + half) * 2 + core) * rows
                first = at + side * rows
                w_ref[pl.ds(pl.multiple_of(start, 8), rows), :count] = ref[first : first + rows, :]
    whole = w_ref[...].astype(jnp.float32)
    scale_ref[...] = lax.rsqrt(jnp.sum(whole * whole, 0, keepdims=True) + epsilon)


def join_kernel(*refs):
    *pieces, out_ref = refs
    at = 0
    for piece in pieces:
        out_ref[at : at + piece.shape[0], :] = piece[...]
        at += piece.shape[0]


def join(*pieces):
    vmem = pl.BlockSpec(memory_space=pltpu.VMEM)
    rows, wide = sum(piece.shape[0] for piece in pieces), pieces[0].shape[1]
    return pl.pallas_call(
        join_kernel,
        name="join",
        out_shape=jax.ShapeDtypeStruct((rows, wide), pieces[0].dtype),
        in_specs=[vmem] * len(pieces),
        out_specs=vmem,
        compiler_params=pltpu.CompilerParams(vmem_limit_bytes=JOIN_VMEM),
        cost_estimate=pl.CostEstimate(flops=rows * wide, bytes_accessed=4 * rows * wide, transcendentals=0),
    )(*pieces)


def with_ids(docs, ids):
    size, wide = docs.shape
    row = lax.broadcasted_iota(jnp.int32, (size + 8, wide), 0)
    ids = jnp.pad(ids, (0, wide - size))[None, :]
    digits = jnp.where(row == size, ids >> 7, jnp.where(row == size + 1, ids & 127, 0))
    return jnp.where(row < size, jnp.pad(docs, ((0, 8), (0, 0))), digits.astype(docs.dtype))


def score_kernel(count, *refs):
    *blocks, w_ref, scale_ref, out_ref, rows_ref, ids_ref, best_ref, chosen_ref = refs
    first = (lax.axis_index("y") * 2 + lax.axis_index("xl")) * count
    size = out_ref.shape[1]
    for k, block in enumerate(blocks):
        here = slice(k * size, (k + 1) * size)
        rows_ref[here, :] = block[:size, :]
        digits = block[size : size + 8, :size].astype(jnp.float32)
        ids = digits[0:1] * 128.0 + digits[1:2] - first.astype(jnp.float32)
        ids_ref[here, :] = jnp.broadcast_to(ids, (LANES, size)).T
    wide = w_ref.shape[1]
    lane = lax.broadcasted_iota(jnp.int32, (1, LANES), 1).astype(jnp.float32)
    for start in range(0, wide, CHUNK):
        stop = min(start + CHUNK, wide)
        products = jnp.dot(rows_ref[...], w_ref[:, start:stop], preferred_element_type=jnp.float32)
        scaled = products * scale_ref[:, start:stop]
        for at in range(start, stop, LANES):
            part = scaled[:, at - start : at - start + LANES]
            seen = part
            if at + LANES > count:
                seen = jnp.where(lane < float(count - at), part, LOWEST)
            hit = ids_ref[...] == lane + float(at)
            if at == 0:
                best_ref[...] = seen
                chosen_ref[...] = jnp.where(hit, seen, LOWEST)
            else:
                best_ref[...] = jnp.maximum(best_ref[...], seen)
                chosen_ref[...] = jnp.where(hit, seen, chosen_ref[...])
    for k in range(len(blocks)):
        here = slice(k * size, (k + 1) * size)
        out_ref[2 * k : 2 * k + 1, :] = jnp.max(best_ref[here, :].T, 0, keepdims=True)
        out_ref[2 * k + 1 : 2 * k + 2, :] = jnp.max(chosen_ref[here, :].T, 0, keepdims=True)


def score(blocks, w, scale, count, size):
    n = len(blocks)
    vmem = pl.BlockSpec(memory_space=pltpu.VMEM)
    return pl.pallas_call(
        lambda *refs: score_kernel(count, *refs),
        name="score",
        out_shape=jax.ShapeDtypeStruct((2 * n, size), jnp.float32),
        in_specs=[vmem] * (n + 2),
        out_specs=vmem,
        scratch_shapes=[
            pltpu.VMEM((n * size, w.shape[0]), jnp.bfloat16),
            pltpu.VMEM((n * size, LANES), jnp.float32),
            pltpu.VMEM((n * size, LANES), jnp.float32),
            pltpu.VMEM((n * size, LANES), jnp.float32),
        ],
        compiler_params=pltpu.CompilerParams(vmem_limit_bytes=SCORE_VMEM),
        cost_estimate=pl.CostEstimate(
            flops=2 * n * size * w.shape[0] * w.shape[1], bytes_accessed=n * size * w.shape[0] * 2, transcendentals=0
        ),
    )(*blocks, w, scale)


def whole_block(pieces, early, late):
    vmem = pl.BlockSpec(memory_space=pltpu.VMEM)
    height, count = pieces[0].shape
    wide = -(-count // LANES) * LANES
    return pl.pallas_call(
        assemble_kernel,
        name="assemble",
        out_shape=(
            jax.ShapeDtypeStruct((16 * height, wide), jnp.bfloat16),
            jax.ShapeDtypeStruct((1, wide), jnp.float32),
        ),
        in_specs=[vmem] * (len(pieces) + 2),
        out_specs=(vmem, vmem),
        compiler_params=pltpu.CompilerParams(vmem_limit_bytes=ASSEMBLE_VMEM),
        cost_estimate=pl.CostEstimate(flops=16 * height * wide, bytes_accessed=32 * height * wide, transcendentals=0),
    )(*pieces, early, late)


def on_device(sizes, docs, centroids, assigned):
    def send(value, move):
        return lax.ppermute(value, ALL, hops(sizes, move))

    size, _ = docs.shape
    count = centroids.shape[0]
    part = centroids.T
    theirs = send(part, far_x)
    mine = join(part)
    own = with_ids(docs, assigned)
    rows = [own, send(own, first_y), send(own, second_y)]
    rows.append(send(rows[1], second_y))
    pairs = [send(rows[k], across_x) for k in range(3)]
    pairs.append(send(rows[1], both_ways))
    both = join(mine, theirs)
    two, back_two = send(both, along_z(2)), send(both, along_z(-2))
    one, back_one = send(both, along_z(1)), send(both, along_z(-1))
    three, back_three = send(two, along_z(1)), send(back_two, along_z(-1))
    four = send(two, along_z(2))
    slices = [both, one, back_one, two, back_two, three, back_three, four]
    early = send(join(*slices[:5]), other_core)
    late = send(join(*slices[5:]), other_core)
    w, scale = whole_block(slices, early, late)
    wide = docs.astype(jnp.float32)
    scale_x = lax.rsqrt(jnp.sum(wide * wide, 1) + epsilon)
    away = send(score([pairs[k] for k in (1, 3, 0, 2)], w, scale, count, size), across_x)
    give = jnp.maximum(score([rows[1], rows[3]], w, scale, count, size), away[:4])
    got = send(give, first_y)
    keep = jnp.maximum(score([rows[0], rows[2]], w, scale, count, size), away[4:])
    keep = jnp.maximum(keep, got)
    total = jnp.maximum(keep[:2], send(keep[2:], second_y))
    nearest, chosen = (1.0 - total[k] * scale_x for k in (0, 1))
    return (nearest, chosen)


def solution(mesh):
    clu, doc = mesh.shape["clu"], mesh.shape["doc"]
    sizes = (clu // 4, 2, 2, doc // 2, 2)
    torus = Mesh(mesh.devices.reshape(sizes), AXES)
    placed = (P(ALL, None), P(DOC, CLU), P(ALL))


    def body(*args):
        return on_device(sizes, *args)

    return jax.shard_map(body, mesh=torus, in_specs=placed, out_specs=(P(ALL), P(ALL)), check_vma=False)
```

```python
import itertools

import jax
import jax.numpy as jnp
from jax import lax
from jax.experimental import pallas as pl
from jax.experimental.pallas import tpu as pltpu
from jax.sharding import Mesh
from jax.sharding import PartitionSpec as P

AXES = ("z", "xh", "c", "y", "xl")
DOC = ("y", "xl")
CLU = ("z", "xh", "c")
ALL = ("z", "xh", "c", "y", "xl")


epsilon = 1e-06
LOWEST = -3.0e38
LANES = 128
CHUNK = 256
SCORE_VMEM = 16 << 20
ASSEMBLE_VMEM = 16 << 20
JOIN_VMEM = 4 << 20
AHEAD = 4_000_000_000
STEPS = (0, 1, -1, 2, -2, 3, -3, 4)


def hops(sizes, move):
    pairs = []
    for here in itertools.product(*(range(n) for n in sizes)):
        there = move(*here)
        index = [0, 0]
        for n, a, b in zip(sizes, here, there):
            index = [index[0] * n + a, index[1] * n + b % n]
        pairs.append(tuple(index))
    return pairs


def way(c):
    return 1 - 2 * c


def along_z(step):
    return lambda z, xh, c, y, xl: (z + step * way(c), xh, c, y, xl)


def across_x(z, xh, c, y, xl):
    x = 2 * xh + xl
    other = x + 1 if (x + c) % 2 == 0 else x - 1
    other %= 4
    return (z, other // 2, c, y, other % 2)


def far_x(z, xh, c, y, xl):
    return (z, xh + 1, c, y, xl)


def first_y(z, xh, c, y, xl):
    return (z, xh, c, (3 - y) if c else y + 1 - 2 * (y % 2), xl)


def second_y(z, xh, c, y, xl):
    return (z, xh, c, y + 1 - 2 * (y % 2) if c else (3 - y), xl)


def both_ways(*place):
    return second_y(*across_x(*place))


def other_core(z, xh, c, y, xl):
    return (z, xh, c + 1, y, xl)


def assemble_kernel(*refs):
    *pieces, early_ref, late_ref, w_ref, scale_ref = refs
    z, xh, c = (lax.axis_index(name) for name in CLU)
    deep, wide = w_ref.shape
    height, count = pieces[0].shape
    rows = height // 2
    w_ref[:, count - count % LANES :] = jnp.zeros((deep, wide - count + count % LANES), w_ref.dtype)
    traded = [(ref, k * height) for ref in (early_ref, late_ref) for k in range(ref.shape[0] // height)]
    for core, arrived in ((c, [(ref, 0) for ref in pieces]), (1 - c, traded)):
        for step, (ref, at) in zip(STEPS, arrived):
            level = lax.rem(z - way(core) * step + 8, 8)
            for side in (0, 1):
                half = side + xh - 2 * side * xh
                start = ((level * 2 + half) * 2 + core) * rows
                first = at + side * rows
                w_ref[pl.ds(pl.multiple_of(start, 8), rows), :count] = ref[first : first + rows, :]
    whole = w_ref[...].astype(jnp.float32)
    scale_ref[...] = lax.rsqrt(jnp.sum(whole * whole, 0, keepdims=True) + epsilon)


def join_kernel(*refs):
    *pieces, out_ref = refs
    at = 0
    for piece in pieces:
        out_ref[at : at + piece.shape[0], :] = piece[...]
        at += piece.shape[0]


def join(*pieces):
    vmem = pl.BlockSpec(memory_space=pltpu.VMEM)
    rows, wide = sum(piece.shape[0] for piece in pieces), pieces[0].shape[1]
    return pl.pallas_call(
        join_kernel,
        name="join",
        out_shape=jax.ShapeDtypeStruct((rows, wide), pieces[0].dtype),
        in_specs=[vmem] * len(pieces),
        out_specs=vmem,
        compiler_params=pltpu.CompilerParams(vmem_limit_bytes=JOIN_VMEM),
        cost_estimate=pl.CostEstimate(flops=rows * wide, bytes_accessed=4 * rows * wide, transcendentals=0),
    )(*pieces)


def blank_kernel(out_ref):
    out_ref[...] = jnp.zeros_like(out_ref)


def blank(rows, wide, dtype):
    return pl.pallas_call(
        blank_kernel,
        name="blank",
        out_shape=jax.ShapeDtypeStruct((rows, wide), dtype),
        out_specs=pl.BlockSpec(memory_space=pltpu.VMEM),
        compiler_params=pltpu.CompilerParams(vmem_limit_bytes=JOIN_VMEM),
        cost_estimate=pl.CostEstimate(flops=AHEAD, bytes_accessed=4 * rows * wide, transcendentals=0),
    )()


def with_ids_kernel(docs_ref, ids_ref, tail_ref, out_ref):
    size, _ = docs_ref.shape
    out_ref[:size, :] = docs_ref[...]
    out_ref[size:, :] = tail_ref[...]
    ids = ids_ref[...]
    digit = lax.broadcasted_iota(jnp.int32, (tail_ref.shape[0], size), 0)
    digits = jnp.where(digit == 0, ids >> 7, jnp.where(digit == 1, ids & 127, 0))
    out_ref[size:, :size] = digits.astype(jnp.float32).astype(out_ref.dtype)


def with_ids(docs, ids, tail):
    vmem = pl.BlockSpec(memory_space=pltpu.VMEM)
    return pl.pallas_call(
        with_ids_kernel,
        name="with_ids",
        out_shape=jax.ShapeDtypeStruct((docs.shape[0] + tail.shape[0], docs.shape[1]), docs.dtype),
        in_specs=[vmem] * 3,
        out_specs=vmem,
        compiler_params=pltpu.CompilerParams(vmem_limit_bytes=JOIN_VMEM),
        cost_estimate=pl.CostEstimate(flops=docs.size, bytes_accessed=4 * docs.size, transcendentals=0),
    )(docs, ids.reshape(1, -1), tail)


def score_kernel(count, *refs):
    *blocks, w_ref, scale_ref, out_ref, rows_ref, ids_ref, best_ref, chosen_ref = refs
    first = (lax.axis_index("y") * 2 + lax.axis_index("xl")) * count
    size = out_ref.shape[1]
    for k, block in enumerate(blocks):
        here = slice(k * size, (k + 1) * size)
        rows_ref[here, :] = block[:size, :]
        digits = block[size : size + 8, :size].astype(jnp.float32)
        ids = digits[0:1] * 128.0 + digits[1:2] - first.astype(jnp.float32)
        ids_ref[here, :] = jnp.broadcast_to(ids, (LANES, size)).T
    wide = w_ref.shape[1]
    lane = lax.broadcasted_iota(jnp.int32, (1, LANES), 1).astype(jnp.float32)
    for start in range(0, wide, CHUNK):
        stop = min(start + CHUNK, wide)
        products = jnp.dot(rows_ref[...], w_ref[:, start:stop], preferred_element_type=jnp.float32)
        scaled = products * scale_ref[:, start:stop]
        for at in range(start, stop, LANES):
            part = scaled[:, at - start : at - start + LANES]
            seen = part
            if at + LANES > count:
                seen = jnp.where(lane < float(count - at), part, LOWEST)
            hit = ids_ref[...] == lane + float(at)
            if at == 0:
                best_ref[...] = seen
                chosen_ref[...] = jnp.where(hit, seen, LOWEST)
            else:
                best_ref[...] = jnp.maximum(best_ref[...], seen)
                chosen_ref[...] = jnp.where(hit, seen, chosen_ref[...])
    for k in range(len(blocks)):
        here = slice(k * size, (k + 1) * size)
        out_ref[2 * k : 2 * k + 1, :] = jnp.max(best_ref[here, :].T, 0, keepdims=True)
        out_ref[2 * k + 1 : 2 * k + 2, :] = jnp.max(chosen_ref[here, :].T, 0, keepdims=True)


def score(blocks, w, scale, count, size):
    n = len(blocks)
    vmem = pl.BlockSpec(memory_space=pltpu.VMEM)
    return pl.pallas_call(
        lambda *refs: score_kernel(count, *refs),
        name="score",
        out_shape=jax.ShapeDtypeStruct((2 * n, size), jnp.float32),
        in_specs=[vmem] * (n + 2),
        out_specs=vmem,
        scratch_shapes=[
            pltpu.VMEM((n * size, w.shape[0]), jnp.bfloat16),
            pltpu.VMEM((n * size, LANES), jnp.float32),
            pltpu.VMEM((n * size, LANES), jnp.float32),
            pltpu.VMEM((n * size, LANES), jnp.float32),
        ],
        compiler_params=pltpu.CompilerParams(vmem_limit_bytes=SCORE_VMEM),
        cost_estimate=pl.CostEstimate(
            flops=2 * n * size * w.shape[0] * w.shape[1], bytes_accessed=n * size * w.shape[0] * 2, transcendentals=0
        ),
    )(*blocks, w, scale)


def whole_block(pieces, early, late):
    vmem = pl.BlockSpec(memory_space=pltpu.VMEM)
    height, count = pieces[0].shape
    wide = -(-count // LANES) * LANES
    return pl.pallas_call(
        assemble_kernel,
        name="assemble",
        out_shape=(
            jax.ShapeDtypeStruct((16 * height, wide), jnp.bfloat16),
            jax.ShapeDtypeStruct((1, wide), jnp.float32),
        ),
        in_specs=[vmem] * (len(pieces) + 2),
        out_specs=(vmem, vmem),
        compiler_params=pltpu.CompilerParams(vmem_limit_bytes=ASSEMBLE_VMEM),
        cost_estimate=pl.CostEstimate(flops=16 * height * wide, bytes_accessed=32 * height * wide, transcendentals=0),
    )(*pieces, early, late)


def on_device(sizes, docs, centroids, assigned):
    def send(value, move):
        return lax.ppermute(value, ALL, hops(sizes, move))

    size, _ = docs.shape
    count = centroids.shape[0]
    part = centroids.T
    theirs = send(part, far_x)
    tail = blank(8, docs.shape[1], docs.dtype)
    own = with_ids(docs, assigned, tail)
    rows = [own, send(own, first_y), send(own, second_y)]
    rows.append(send(rows[1], second_y))
    pairs = [send(rows[k], across_x) for k in range(3)]
    pairs.append(send(rows[1], both_ways))
    both = join(part, theirs)
    two, back_two = send(both, along_z(2)), send(both, along_z(-2))
    one, back_one = send(both, along_z(1)), send(both, along_z(-1))
    three, back_three = send(two, along_z(1)), send(back_two, along_z(-1))
    four = send(two, along_z(2))
    slices = [both, one, back_one, two, back_two, three, back_three, four]
    early = send(join(*slices[:5]), other_core)
    late = send(join(*slices[5:]), other_core)
    w, scale = whole_block(slices, early, late)
    wide = docs.astype(jnp.float32)
    scale_x = lax.rsqrt(jnp.sum(wide * wide, 1) + epsilon)
    away = send(score([pairs[k] for k in (1, 3, 0, 2)], w, scale, count, size), across_x)
    give = jnp.maximum(score([rows[1], rows[3]], w, scale, count, size), away[:4])
    got = send(give, first_y)
    keep = jnp.maximum(score([rows[0], rows[2]], w, scale, count, size), away[4:])
    keep = jnp.maximum(keep, got)
    total = jnp.maximum(keep[:2], send(keep[2:], second_y))
    nearest, chosen = (1.0 - total[k] * scale_x for k in (0, 1))
    return (nearest, chosen)


def solution(mesh):
    clu, doc = mesh.shape["clu"], mesh.shape["doc"]
    sizes = (clu // 4, 2, 2, doc // 2, 2)
    torus = Mesh(mesh.devices.reshape(sizes), AXES)
    placed = (P(ALL, None), P(DOC, CLU), P(ALL))


    def body(*args):
        return on_device(sizes, *args)

    return jax.shard_map(body, mesh=torus, in_specs=placed, out_specs=(P(ALL), P(ALL)), check_vma=False)
```

```python
import itertools

import jax
import jax.numpy as jnp
from jax import lax
from jax.experimental import pallas as pl
from jax.experimental.pallas import tpu as pltpu
from jax.sharding import Mesh
from jax.sharding import PartitionSpec as P

AXES = ("z", "xh", "c", "y", "xl")
DOC = ("y", "xl")
CLU = ("z", "xh", "c")
ALL = ("z", "xh", "c", "y", "xl")


epsilon = 1e-06
LOWEST = -3.0e38
LANES = 128
CHUNK = 512
SCORE_VMEM = 16 << 20
ASSEMBLE_VMEM = 16 << 20
JOIN_VMEM = 4 << 20
AHEAD = 4_000_000_000
STEPS = (0, 1, -1, 2, -2, 4, 3, -3)


def hops(sizes, move):
    pairs = []
    for here in itertools.product(*(range(n) for n in sizes)):
        there = move(*here)
        index = [0, 0]
        for n, a, b in zip(sizes, here, there):
            index = [index[0] * n + a, index[1] * n + b % n]
        pairs.append(tuple(index))
    return pairs


def way(c):
    return 1 - 2 * c


def along_z(step):
    return lambda z, xh, c, y, xl: (z + step * way(c), xh, c, y, xl)


def across_x(z, xh, c, y, xl):
    x = 2 * xh + xl
    other = x + 1 if (x + c) % 2 == 0 else x - 1
    other %= 4
    return (z, other // 2, c, y, other % 2)


def far_x(z, xh, c, y, xl):
    return (z, xh + 1, c, y, xl)


def first_y(z, xh, c, y, xl):
    return (z, xh, c, (3 - y) if c else y + 1 - 2 * (y % 2), xl)


def second_y(z, xh, c, y, xl):
    return (z, xh, c, y + 1 - 2 * (y % 2) if c else (3 - y), xl)


def both_ways(*place):
    return second_y(*across_x(*place))


def other_core(z, xh, c, y, xl):
    return (z, xh, c + 1, y, xl)


def rows_of(core, step, side, rows):
    z, xh = lax.axis_index("z"), lax.axis_index("xh")
    level = lax.rem(z - way(core) * step + 8, 8)
    half = side + xh - 2 * side * xh
    return pl.ds(pl.multiple_of(((level * 2 + half) * 2 + core) * rows, 8), rows)


def sum_of_squares(values):
    wide = values.astype(jnp.float32)
    return jnp.sum(wide * wide, 0, keepdims=True)


def assemble_kernel(*refs):
    *pieces, traded_ref, w_ref, squares_ref = refs
    c = lax.axis_index("c")
    deep, wide = w_ref.shape
    height, count = pieces[0].shape
    rows = height // 2
    w_ref[:, count - count % LANES :] = jnp.zeros((deep, wide - count + count % LANES), w_ref.dtype)
    for k, step in enumerate(STEPS):
        for side in (0, 1):
            first = side * rows
            w_ref[rows_of(c, step, side, rows), :count] = pieces[k][first : first + rows, :]
            if k * height < traded_ref.shape[0]:
                first += k * height
                part = traded_ref[first : first + rows, :]
            else:
                part = jnp.zeros((rows, count), w_ref.dtype)
            w_ref[rows_of(1 - c, step, side, rows), :count] = part
    squares_ref[...] = sum_of_squares(w_ref[...])


def complete_kernel(before_ref, squares_ref, late_ref, w_ref, scale_ref):
    c = lax.axis_index("c")
    count = late_ref.shape[1]
    rows = before_ref.shape[0] // 32
    height = 2 * rows
    late = late_ref.shape[0] // height
    for k, step in enumerate(STEPS[8 - late :]):
        for side in (0, 1):
            first = k * height + side * rows
            w_ref[rows_of(1 - c, step, side, rows), :count] = late_ref[first : first + rows, :]
    squares = squares_ref[...]
    scale_ref[...] = lax.rsqrt(squares + epsilon)
    scale_ref[:, :count] = lax.rsqrt(squares[:, :count] + sum_of_squares(late_ref[...]) + epsilon)


def join_kernel(*refs):
    *pieces, out_ref = refs
    at = 0
    for piece in pieces:
        out_ref[at : at + piece.shape[0], :] = piece[...]
        at += piece.shape[0]


def join(*pieces):
    vmem = pl.BlockSpec(memory_space=pltpu.VMEM)
    rows, wide = sum(piece.shape[0] for piece in pieces), pieces[0].shape[1]
    return pl.pallas_call(
        join_kernel,
        name="join",
        out_shape=jax.ShapeDtypeStruct((rows, wide), pieces[0].dtype),
        in_specs=[vmem] * len(pieces),
        out_specs=vmem,
        compiler_params=pltpu.CompilerParams(vmem_limit_bytes=JOIN_VMEM),
        cost_estimate=pl.CostEstimate(flops=rows * wide, bytes_accessed=4 * rows * wide, transcendentals=0),
    )(*pieces)


def blank_kernel(out_ref):
    out_ref[...] = jnp.zeros_like(out_ref)


def blank(rows, wide, dtype):
    return pl.pallas_call(
        blank_kernel,
        name="blank",
        out_shape=jax.ShapeDtypeStruct((rows, wide), dtype),
        out_specs=pl.BlockSpec(memory_space=pltpu.VMEM),
        compiler_params=pltpu.CompilerParams(vmem_limit_bytes=JOIN_VMEM),
        cost_estimate=pl.CostEstimate(flops=AHEAD, bytes_accessed=4 * rows * wide, transcendentals=0),
    )()


def with_ids_kernel(docs_ref, ids_ref, tail_ref, out_ref):
    size, _ = docs_ref.shape
    out_ref[:size, :] = docs_ref[...]
    out_ref[size:, :] = tail_ref[...]
    ids = ids_ref[...]
    digit = lax.broadcasted_iota(jnp.int32, (tail_ref.shape[0], size), 0)
    digits = jnp.where(digit == 0, ids >> 7, jnp.where(digit == 1, ids & 127, 0))
    out_ref[size:, :size] = digits.astype(jnp.float32).astype(out_ref.dtype)


def with_ids(docs, ids, tail):
    vmem = pl.BlockSpec(memory_space=pltpu.VMEM)
    return pl.pallas_call(
        with_ids_kernel,
        name="with_ids",
        out_shape=jax.ShapeDtypeStruct((docs.shape[0] + tail.shape[0], docs.shape[1]), docs.dtype),
        in_specs=[vmem] * 3,
        out_specs=vmem,
        compiler_params=pltpu.CompilerParams(vmem_limit_bytes=JOIN_VMEM),
        cost_estimate=pl.CostEstimate(flops=docs.size, bytes_accessed=4 * docs.size, transcendentals=0),
    )(docs, ids.reshape(1, -1), tail)


def score_kernel(count, *refs):
    *blocks, w_ref, scale_ref, out_ref, rows_ref, ids_ref, best_ref, chosen_ref = refs
    first = (lax.axis_index("y") * 2 + lax.axis_index("xl")) * count
    size = out_ref.shape[1]
    for k, block in enumerate(blocks):
        here = slice(k * size, (k + 1) * size)
        rows_ref[here, :] = block[:size, :]
        digits = block[size : size + 8, :size].astype(jnp.float32)
        ids = digits[0:1] * 128.0 + digits[1:2] - first.astype(jnp.float32)
        ids_ref[here, :] = jnp.broadcast_to(ids, (LANES, size)).T
    wide = w_ref.shape[1]
    lane = lax.broadcasted_iota(jnp.int32, (1, LANES), 1).astype(jnp.float32)
    for start in range(0, wide, CHUNK):
        stop = min(start + CHUNK, wide)
        products = jnp.dot(rows_ref[...], w_ref[:, start:stop], preferred_element_type=jnp.float32)
        scaled = products * scale_ref[:, start:stop]
        best = None if start == 0 else best_ref[...]
        chosen = LOWEST if start == 0 else chosen_ref[...]
        ids = ids_ref[...]
        for at in range(start, stop, LANES):
            part = scaled[:, at - start : at - start + LANES]
            if at + LANES > count:
                part = jnp.where(lane < float(count - at), part, LOWEST)
            best = part if best is None else jnp.maximum(best, part)
            chosen = jnp.where(ids == lane + float(at), part, chosen)
        best_ref[...] = best
        chosen_ref[...] = chosen
    for k in range(len(blocks)):
        here = slice(k * size, (k + 1) * size)
        out_ref[2 * k : 2 * k + 1, :] = jnp.max(best_ref[here, :].T, 0, keepdims=True)
        out_ref[2 * k + 1 : 2 * k + 2, :] = jnp.max(chosen_ref[here, :].T, 0, keepdims=True)


def score(blocks, w, scale, count, size):
    n = len(blocks)
    vmem = pl.BlockSpec(memory_space=pltpu.VMEM)
    return pl.pallas_call(
        lambda *refs: score_kernel(count, *refs),
        name="score",
        out_shape=jax.ShapeDtypeStruct((2 * n, size), jnp.float32),
        in_specs=[vmem] * (n + 2),
        out_specs=vmem,
        scratch_shapes=[
            pltpu.VMEM((n * size, w.shape[0]), jnp.bfloat16),
            pltpu.VMEM((n * size, LANES), jnp.float32),
            pltpu.VMEM((n * size, LANES), jnp.float32),
            pltpu.VMEM((n * size, LANES), jnp.float32),
        ],
        compiler_params=pltpu.CompilerParams(vmem_limit_bytes=SCORE_VMEM),
        cost_estimate=pl.CostEstimate(
            flops=2 * n * size * w.shape[0] * w.shape[1], bytes_accessed=n * size * w.shape[0] * 2, transcendentals=0
        ),
    )(*blocks, w, scale)


def whole_block(pieces, early, late):
    vmem = pl.BlockSpec(memory_space=pltpu.VMEM)
    height, count = pieces[0].shape
    deep, wide = 16 * height, -(-count // LANES) * LANES
    block, line = jax.ShapeDtypeStruct((deep, wide), jnp.bfloat16), jax.ShapeDtypeStruct((1, wide), jnp.float32)
    params = pltpu.CompilerParams(vmem_limit_bytes=ASSEMBLE_VMEM)
    most, squares = pl.pallas_call(
        assemble_kernel,
        name="assemble",
        out_shape=(block, line),
        in_specs=[vmem] * (len(pieces) + 1),
        out_specs=(vmem, vmem),
        compiler_params=params,
        cost_estimate=pl.CostEstimate(flops=2 * deep * wide, bytes_accessed=4 * deep * wide, transcendentals=0),
    )(*pieces, early)
    return pl.pallas_call(
        complete_kernel,
        name="complete",
        out_shape=(block, line),
        in_specs=[vmem] * 3,
        out_specs=(vmem, vmem),
        input_output_aliases={0: 0},
        compiler_params=params,
        cost_estimate=pl.CostEstimate(flops=2 * late.size, bytes_accessed=4 * late.size, transcendentals=wide),
    )(most, squares, late)


def on_device(sizes, docs, centroids, assigned):
    def send(value, move):
        return lax.ppermute(value, ALL, hops(sizes, move))

    size, _ = docs.shape
    count = centroids.shape[0]
    part = centroids.T
    theirs = send(part, far_x)
    tail = blank(8, docs.shape[1], docs.dtype)
    own = with_ids(docs, assigned, tail)
    rows = [own, send(own, first_y), send(own, second_y)]
    rows.append(send(rows[1], second_y))
    pairs = [send(own, across_x), send(rows[1], across_x)]
    pairs += [send(pairs[0], second_y), send(rows[1], both_ways)]
    both = join(part, theirs)
    two, back_two = send(both, along_z(2)), send(both, along_z(-2))
    one, back_one = send(both, along_z(1)), send(both, along_z(-1))
    three, back_three = send(two, along_z(1)), send(back_two, along_z(-1))
    four = send(two, along_z(2))
    slices = [both, one, back_one, two, back_two, four, three, back_three]
    early = send(join(*slices[:5]), other_core)
    late = send(join(*slices[5:]), other_core)
    w, scale = whole_block(slices, early, late)
    wide = docs.astype(jnp.float32)
    scale_x = lax.rsqrt(jnp.sum(wide * wide, 1) + epsilon)
    away = send(score([pairs[k] for k in (1, 3, 0, 2)], w, scale, count, size), across_x)
    give = jnp.maximum(score([rows[1], rows[3]], w, scale, count, size), away[:4])
    got = send(give, first_y)
    keep = jnp.maximum(score([rows[0], rows[2]], w, scale, count, size), away[4:])
    keep = jnp.maximum(keep, got)
    total = jnp.maximum(keep[:2], send(keep[2:], second_y))
    nearest, chosen = (1.0 - total[k] * scale_x for k in (0, 1))
    return (nearest, chosen)


def solution(mesh):
    clu, doc = mesh.shape["clu"], mesh.shape["doc"]
    sizes = (clu // 4, 2, 2, doc // 2, 2)
    torus = Mesh(mesh.devices.reshape(sizes), AXES)
    placed = (P(ALL, None), P(DOC, CLU), P(ALL))


    def body(*args):
        return on_device(sizes, *args)

    return jax.shard_map(body, mesh=torus, in_specs=placed, out_specs=(P(ALL), P(ALL)), check_vma=False)
```

```python
import itertools

import jax
import jax.numpy as jnp
from jax import lax
from jax.experimental import pallas as pl
from jax.experimental.pallas import tpu as pltpu
from jax.sharding import Mesh
from jax.sharding import PartitionSpec as P

AXES = ("z", "xh", "c", "y", "xl")
DOC = ("y", "xl")
CLU = ("z", "xh", "c")
ALL = ("z", "xh", "c", "y", "xl")


epsilon = 1e-06
LOWEST = -3.0e38
LANES = 128
CHUNK = 512
SCORE_VMEM = 16 << 20
ASSEMBLE_VMEM = 16 << 20
JOIN_VMEM = 4 << 20
AHEAD = 4_000_000_000
STEPS = (0, 1, -1, 2, -2, 4, 3, -3)


def hops(sizes, move):
    pairs = []
    for here in itertools.product(*(range(n) for n in sizes)):
        there = move(*here)
        index = [0, 0]
        for n, a, b in zip(sizes, here, there):
            index = [index[0] * n + a, index[1] * n + b % n]
        pairs.append(tuple(index))
    return pairs


def way(c):
    return 1 - 2 * c


def along_z(step):
    return lambda z, xh, c, y, xl: (z + step * way(c), xh, c, y, xl)


def across_x(z, xh, c, y, xl):
    x = 2 * xh + xl
    other = x + 1 if (x + c) % 2 == 0 else x - 1
    other %= 4
    return (z, other // 2, c, y, other % 2)


def far_x(z, xh, c, y, xl):
    return (z, xh + 1, c, y, xl)


def first_y(z, xh, c, y, xl):
    return (z, xh, c, (3 - y) if c else y + 1 - 2 * (y % 2), xl)


def second_y(z, xh, c, y, xl):
    return (z, xh, c, y + 1 - 2 * (y % 2) if c else (3 - y), xl)


def both_ways(*place):
    return second_y(*across_x(*place))


def other_core(z, xh, c, y, xl):
    return (z, xh, c + 1, y, xl)


def rows_of(core, step, side, rows):
    z, xh = lax.axis_index("z"), lax.axis_index("xh")
    level = lax.rem(z - way(core) * step + 8, 8)
    half = side + xh - 2 * side * xh
    return pl.ds(pl.multiple_of(((level * 2 + half) * 2 + core) * rows, 8), rows)


def sum_of_squares(values):
    wide = values.astype(jnp.float32)
    return jnp.sum(wide * wide, 0, keepdims=True)


def assemble_kernel(*refs):
    *pieces, traded_ref, w_ref, squares_ref = refs
    c = lax.axis_index("c")
    deep, wide = w_ref.shape
    height, count = pieces[0].shape
    rows = height // 2
    w_ref[:, count - count % LANES :] = jnp.zeros((deep, wide - count + count % LANES), w_ref.dtype)
    for k, step in enumerate(STEPS):
        for side in (0, 1):
            first = side * rows
            w_ref[rows_of(c, step, side, rows), :count] = pieces[k][first : first + rows, :]
            if k * height < traded_ref.shape[0]:
                first += k * height
                part = traded_ref[first : first + rows, :]
            else:
                part = jnp.zeros((rows, count), w_ref.dtype)
            w_ref[rows_of(1 - c, step, side, rows), :count] = part
    squares_ref[...] = sum_of_squares(w_ref[...])


def complete_kernel(before_ref, squares_ref, late_ref, w_ref, scale_ref):
    c = lax.axis_index("c")
    count = late_ref.shape[1]
    rows = before_ref.shape[0] // 32
    height = 2 * rows
    late = late_ref.shape[0] // height
    for k, step in enumerate(STEPS[8 - late :]):
        for side in (0, 1):
            first = k * height + side * rows
            w_ref[rows_of(1 - c, step, side, rows), :count] = late_ref[first : first + rows, :]
    squares = squares_ref[...]
    scale_ref[...] = lax.rsqrt(squares + epsilon)
    scale_ref[:, :count] = lax.rsqrt(squares[:, :count] + sum_of_squares(late_ref[...]) + epsilon)


def join_kernel(*refs):
    *pieces, out_ref = refs
    at = 0
    for piece in pieces:
        out_ref[at : at + piece.shape[0], :] = piece[...]
        at += piece.shape[0]


def join(*pieces):
    vmem = pl.BlockSpec(memory_space=pltpu.VMEM)
    rows, wide = sum(piece.shape[0] for piece in pieces), pieces[0].shape[1]
    return pl.pallas_call(
        join_kernel,
        name="join",
        out_shape=jax.ShapeDtypeStruct((rows, wide), pieces[0].dtype),
        in_specs=[vmem] * len(pieces),
        out_specs=vmem,
        compiler_params=pltpu.CompilerParams(vmem_limit_bytes=JOIN_VMEM),
        cost_estimate=pl.CostEstimate(flops=rows * wide, bytes_accessed=4 * rows * wide, transcendentals=0),
    )(*pieces)


def blank_kernel(out_ref):
    out_ref[...] = jnp.zeros_like(out_ref)


def blank(rows, wide, dtype):
    return pl.pallas_call(
        blank_kernel,
        name="blank",
        out_shape=jax.ShapeDtypeStruct((rows, wide), dtype),
        out_specs=pl.BlockSpec(memory_space=pltpu.VMEM),
        compiler_params=pltpu.CompilerParams(vmem_limit_bytes=JOIN_VMEM),
        cost_estimate=pl.CostEstimate(flops=AHEAD, bytes_accessed=4 * rows * wide, transcendentals=0),
    )()


def with_ids_kernel(docs_ref, ids_ref, tail_ref, out_ref):
    size, _ = docs_ref.shape
    out_ref[:size, :] = docs_ref[...]
    out_ref[size:, :] = tail_ref[...]
    ids = ids_ref[...]
    digit = lax.broadcasted_iota(jnp.int32, (tail_ref.shape[0], size), 0)
    digits = jnp.where(digit == 0, ids >> 7, jnp.where(digit == 1, ids & 127, 0))
    out_ref[size:, :size] = digits.astype(jnp.float32).astype(out_ref.dtype)


def with_ids(docs, ids, tail):
    vmem = pl.BlockSpec(memory_space=pltpu.VMEM)
    return pl.pallas_call(
        with_ids_kernel,
        name="with_ids",
        out_shape=jax.ShapeDtypeStruct((docs.shape[0] + tail.shape[0], docs.shape[1]), docs.dtype),
        in_specs=[vmem] * 3,
        out_specs=vmem,
        compiler_params=pltpu.CompilerParams(vmem_limit_bytes=JOIN_VMEM),
        cost_estimate=pl.CostEstimate(flops=docs.size, bytes_accessed=4 * docs.size, transcendentals=0),
    )(docs, ids.reshape(1, -1), tail)


def stage(count, size, blocks, rows_ref, ids_ref):
    first = (lax.axis_index("y") * 2 + lax.axis_index("xl")) * count
    for k, block in enumerate(blocks):
        here = slice(k * size, (k + 1) * size)
        rows_ref[here, :] = block[:size, :]
        digits = block[size : size + 8, :size].astype(jnp.float32)
        ids = digits[0:1] * 128.0 + digits[1:2] - first.astype(jnp.float32)
        ids_ref[here, :] = jnp.broadcast_to(ids, (LANES, size)).T


def stage_kernel(count, size, *refs):
    *blocks, rows_ref, ids_ref = refs
    stage(count, size, blocks, rows_ref, ids_ref)


def score_kernel(count, *refs):
    *blocks, w_ref, scale_ref, out_ref, rows_ref, ids_ref, best_ref, chosen_ref = refs
    stage(count, out_ref.shape[1], blocks, rows_ref, ids_ref)
    rank(count, w_ref, scale_ref, out_ref, rows_ref, ids_ref, best_ref, chosen_ref)


def staged_kernel(count, rows_ref, ids_ref, w_ref, scale_ref, out_ref, best_ref, chosen_ref):
    rank(count, w_ref, scale_ref, out_ref, rows_ref, ids_ref, best_ref, chosen_ref)


def rank(count, w_ref, scale_ref, out_ref, rows_ref, ids_ref, best_ref, chosen_ref):
    size = out_ref.shape[1]
    wide = w_ref.shape[1]
    lane = lax.broadcasted_iota(jnp.int32, (1, LANES), 1).astype(jnp.float32)
    for start in range(0, wide, CHUNK):
        stop = min(start + CHUNK, wide)
        products = jnp.dot(rows_ref[...], w_ref[:, start:stop], preferred_element_type=jnp.float32)
        scaled = products * scale_ref[:, start:stop]
        best = None if start == 0 else best_ref[...]
        chosen = LOWEST if start == 0 else chosen_ref[...]
        ids = ids_ref[...]
        for at in range(start, stop, LANES):
            part = scaled[:, at - start : at - start + LANES]
            if at + LANES > count:
                part = jnp.where(lane < float(count - at), part, LOWEST)
            best = part if best is None else jnp.maximum(best, part)
            chosen = jnp.where(ids == lane + float(at), part, chosen)
        best_ref[...] = best
        chosen_ref[...] = chosen
    for k in range(out_ref.shape[0] // 2):
        here = slice(k * size, (k + 1) * size)
        out_ref[2 * k : 2 * k + 1, :] = jnp.max(best_ref[here, :].T, 0, keepdims=True)
        out_ref[2 * k + 1 : 2 * k + 2, :] = jnp.max(chosen_ref[here, :].T, 0, keepdims=True)


def score_ahead(blocks, w, scale, count, size):
    n = len(blocks)
    vmem = pl.BlockSpec(memory_space=pltpu.VMEM)
    params = pltpu.CompilerParams(vmem_limit_bytes=SCORE_VMEM)
    rows, ids = pl.pallas_call(
        lambda *refs: stage_kernel(count, size, *refs),
        name="stage",
        out_shape=(
            jax.ShapeDtypeStruct((n * size, w.shape[0]), jnp.bfloat16),
            jax.ShapeDtypeStruct((n * size, LANES), jnp.float32),
        ),
        in_specs=[vmem] * n,
        out_specs=(vmem, vmem),
        compiler_params=params,
        cost_estimate=pl.CostEstimate(
            flops=n * size * w.shape[0], bytes_accessed=4 * n * size * w.shape[0], transcendentals=0
        ),
    )(*blocks)
    return pl.pallas_call(
        lambda *refs: staged_kernel(count, *refs),
        name="staged",
        out_shape=jax.ShapeDtypeStruct((2 * n, size), jnp.float32),
        in_specs=[vmem] * 4,
        out_specs=vmem,
        scratch_shapes=[pltpu.VMEM((n * size, LANES), jnp.float32)] * 2,
        compiler_params=params,
        cost_estimate=pl.CostEstimate(
            flops=2 * n * size * w.shape[0] * w.shape[1], bytes_accessed=n * size * w.shape[0] * 2, transcendentals=0
        ),
    )(rows, ids, w, scale)


def score(blocks, w, scale, count, size):
    n = len(blocks)
    vmem = pl.BlockSpec(memory_space=pltpu.VMEM)
    return pl.pallas_call(
        lambda *refs: score_kernel(count, *refs),
        name="score",
        out_shape=jax.ShapeDtypeStruct((2 * n, size), jnp.float32),
        in_specs=[vmem] * (n + 2),
        out_specs=vmem,
        scratch_shapes=[
            pltpu.VMEM((n * size, w.shape[0]), jnp.bfloat16),
            pltpu.VMEM((n * size, LANES), jnp.float32),
            pltpu.VMEM((n * size, LANES), jnp.float32),
            pltpu.VMEM((n * size, LANES), jnp.float32),
        ],
        compiler_params=pltpu.CompilerParams(vmem_limit_bytes=SCORE_VMEM),
        cost_estimate=pl.CostEstimate(
            flops=2 * n * size * w.shape[0] * w.shape[1], bytes_accessed=n * size * w.shape[0] * 2, transcendentals=0
        ),
    )(*blocks, w, scale)


def whole_block(pieces, early, late):
    vmem = pl.BlockSpec(memory_space=pltpu.VMEM)
    height, count = pieces[0].shape
    deep, wide = 16 * height, -(-count // LANES) * LANES
    block, line = jax.ShapeDtypeStruct((deep, wide), jnp.bfloat16), jax.ShapeDtypeStruct((1, wide), jnp.float32)
    params = pltpu.CompilerParams(vmem_limit_bytes=ASSEMBLE_VMEM)
    most, squares = pl.pallas_call(
        assemble_kernel,
        name="assemble",
        out_shape=(block, line),
        in_specs=[vmem] * (len(pieces) + 1),
        out_specs=(vmem, vmem),
        compiler_params=params,
        cost_estimate=pl.CostEstimate(flops=2 * deep * wide, bytes_accessed=4 * deep * wide, transcendentals=0),
    )(*pieces, early)
    return pl.pallas_call(
        complete_kernel,
        name="complete",
        out_shape=(block, line),
        in_specs=[vmem] * 3,
        out_specs=(vmem, vmem),
        input_output_aliases={0: 0},
        compiler_params=params,
        cost_estimate=pl.CostEstimate(flops=2 * late.size, bytes_accessed=4 * late.size, transcendentals=wide),
    )(most, squares, late)


def on_device(sizes, docs, centroids, assigned):
    def send(value, move):
        return lax.ppermute(value, ALL, hops(sizes, move))

    size, _ = docs.shape
    count = centroids.shape[0]
    part = centroids.T
    theirs = send(part, far_x)
    tail = blank(8, docs.shape[1], docs.dtype)
    own = with_ids(docs, assigned, tail)
    rows = [own, send(own, first_y), send(own, second_y)]
    rows.append(send(rows[1], second_y))
    pairs = [send(own, across_x), send(rows[1], across_x)]
    pairs += [send(pairs[0], second_y), send(rows[1], both_ways)]
    both = join(part, theirs)
    two, back_two = send(both, along_z(2)), send(both, along_z(-2))
    one, back_one = send(both, along_z(1)), send(both, along_z(-1))
    three, back_three = send(two, along_z(1)), send(back_two, along_z(-1))
    four = send(two, along_z(2))
    slices = [both, one, back_one, two, back_two, four, three, back_three]
    early = send(join(*slices[:5]), other_core)
    late = send(join(*slices[5:]), other_core)
    w, scale = whole_block(slices, early, late)
    wide = docs.astype(jnp.float32)
    scale_x = lax.rsqrt(jnp.sum(wide * wide, 1) + epsilon)
    away = send(score_ahead([pairs[k] for k in (1, 3, 0, 2)], w, scale, count, size), across_x)
    give = jnp.maximum(score([rows[1], rows[3]], w, scale, count, size), away[:4])
    got = send(give, first_y)
    keep = jnp.maximum(score([rows[0], rows[2]], w, scale, count, size), away[4:])
    keep = jnp.maximum(keep, got)
    total = jnp.maximum(keep[:2], send(keep[2:], second_y))
    nearest, chosen = (1.0 - total[k] * scale_x for k in (0, 1))
    return (nearest, chosen)


def solution(mesh):
    clu, doc = mesh.shape["clu"], mesh.shape["doc"]
    sizes = (clu // 4, 2, 2, doc // 2, 2)
    torus = Mesh(mesh.devices.reshape(sizes), AXES)
    placed = (P(ALL, None), P(DOC, CLU), P(ALL))


    def body(*args):
        return on_device(sizes, *args)

    return jax.shard_map(body, mesh=torus, in_specs=placed, out_specs=(P(ALL), P(ALL)), check_vma=False)
```
